32 devices in a mesh: stn: 4 (over z), tm: 8 (over y, x, core).
Axes of the slice: x: 2, y: 2, z: 4, core: 2. Of those that a mesh axis runs over, the one named last changes fastest.
Arguments:
- voltages: bfloat16 [128, 2, 2, 256, 2048], P('tm', None, None, 'stn'), may hold values from -6 to 6
- taps: float32 [16, 2048], replicated, may hold values from -1.5 to 1.5
- sk_tolerance: float32 [384], P('tm'), may hold values from 0.05 to 0.3
- station_coords: int32 [256, 2], replicated, may hold values from 0 to 1023
- pointings: int32 [256, 2], replicated, may hold values from -64 to 64
- station_flags: int32 [256], replicated, may hold values 0 or 1
Outputs:
- beam_power: float32 [384, 8, 256], P('tm', None, 'stn')
The draws below stay inside these ranges and needn't reach their ends.
All inputs are finite; a program needn't handle non-finite values.
Results may differ from the reference program's by a relative error of at most 0.0045.
Values may be sent and summed in bfloat16 or wider, within the bound.
A program may use at most 128 MiB of HBM per device.

```python
import math
import jax
import jax.numpy as jnp
from jax import lax

F_DEV = 16
STATIONS = 256
NFFT = 2048
CHAN = 384
TAPS = 16
BEAMS = 256
INTEG = 16
S_DEV = 64
FRAMES = 128
N_STN = 4


def plant(drawn, stream_key, low, largest):
    longest = drawn.shape.index(max(drawn.shape))
    spots = []
    for shift in (0, 1):
        where = [jax.random.randint(jax.random.fold_in(stream_key, axis), (), 0, length) for axis, length in enumerate(drawn.shape)]
        where[longest] = (where[longest] + shift) % drawn.shape[longest]
        spots.append(tuple(where))
    return drawn.at[spots[0]].set(low).at[spots[1]].set(largest)


def shard_levels(stream_key, extent, split, least, high):
    factor_of = 1.0
    for dim, blocks in split:
        steps = jax.random.uniform(jax.random.fold_in(jax.random.fold_in(stream_key, 6), dim), (blocks,), jnp.float32, least / len(split), high / len(split))
        factor_of = factor_of * jnp.repeat(jnp.exp(steps), extent[dim] // blocks).reshape((-1,) + (1,) * (len(extent) - 1 - dim))
    return factor_of


def bell_draw(own_key, extent, scale, most, pieces=(), kind=jnp.bfloat16):
    array = scale * jax.random.normal(own_key, extent, jnp.float32)
    if pieces:
        array = array * shard_levels(own_key, extent, pieces, -0.22, 0.18)
    return jnp.clip(array, -most, most).astype(kind)


def setup_inputs(seed: int = 0) -> dict:
    streams_of = jax.random.split(jax.random.key(seed), 7)
    voltages = bell_draw(streams_of[0], (FRAMES, 2, 2, STATIONS, NFFT), 1.0, 6.0, ((0, 8), (3, 4)))
    taps = bell_draw(streams_of[1], (TAPS, NFFT), TAPS ** -0.5, 1.5, (), jnp.float32)
    sk_tolerance = jnp.clip(jnp.exp(math.log(0.3) - 1.7917595 * jax.random.uniform(streams_of[2], (CHAN,), jnp.float32) ** shard_levels(streams_of[2], (CHAN,), ((0, 8),), -0.2, 0.2)), 0.05, 0.3)
    station_coords = plant(jax.random.randint(streams_of[3], (STATIONS, 2), 0, 1024), jax.random.fold_in(streams_of[3], 1), 0, 1023).astype(jnp.int32)
    pointings = plant(jax.random.randint(streams_of[4], (BEAMS, 2), -64, 65), jax.random.fold_in(streams_of[4], 1), -64, 64).astype(jnp.int32)
    station_flags = plant((jax.random.randint(streams_of[5], (STATIONS,), 0, 8) < 1).astype(jnp.int32), jax.random.fold_in(streams_of[5], 1), 0, 1)
    return {"voltages": voltages, "taps": taps, "sk_tolerance": sk_tolerance, "station_coords": station_coords, "pointings": pointings, "station_flags": station_flags}


def fourier_table(channels, points):
    rows = jnp.arange(channels, dtype=jnp.int32)
    columns = jnp.arange(points, dtype=jnp.int32)
    residue = rows[:, None] * columns[None, :] % points
    angle = 2.0 * math.pi / points * residue.astype(jnp.float32)
    factor = 1.0 / math.sqrt(points)
    return jnp.concatenate([jnp.cos(angle) * factor, jnp.sin(angle) * factor], 0).astype(jnp.bfloat16)

def steering(channel_ids, coords, flags, pointings, scale):
    offsets = coords[:, 0:1] * pointings[None, :, 0] + coords[:, 1:2] * pointings[None, :, 1]
    residue = (channel_ids + 1)[:, None, None] * offsets[None, :, :] % 65536
    angle = 2.0 * math.pi / 65536.0 * residue.astype(jnp.float32)
    live_gain = (1 - flags).astype(jnp.float32) * scale
    real_part = (jnp.cos(angle) * live_gain[None, :, None]).astype(jnp.bfloat16)
    imag_part = (jnp.sin(angle) * live_gain[None, :, None]).astype(jnp.bfloat16)
    upper = jnp.concatenate([real_part, imag_part], 2)
    lower = jnp.concatenate([-imag_part, real_part], 2)
    return jnp.stack([upper, lower], 1)

def own_sum(block, taps):
    frames = block.shape[0]
    span = taps.shape[0] - 1
    padded = jnp.pad(block, ((span, 0), (0, 0), (0, 0), (0, 0), (0, 0)))
    return sum((padded[span - tap_index:span - tap_index + frames].astype(jnp.float32) * taps[tap_index] for tap_index in range(taps.shape[0])))

def carried_sum(last_frames, taps):
    span = taps.shape[0] - 1
    padded = jnp.pad(last_frames, ((0, span), (0, 0), (0, 0), (0, 0), (0, 0)))
    return sum((padded[span - tap_index:2 * span - tap_index].astype(jnp.float32) * taps[tap_index] for tap_index in range(1, span + 1)))

def transform(filtered, table):
    frames = filtered.shape[0]
    local = filtered.shape[3]
    points = filtered.shape[-1]
    flat = filtered.reshape(-1, points)
    product = lax.dot_general(table, flat, (((1,), (1,)), ((), ())), preferred_element_type=jnp.float32)
    channels = table.shape[0] // 2
    product = product.reshape(2, channels, frames, 2, 2, local)
    real_out = product[0, :, :, 0] + product[1, :, :, 1]
    imag_out = product[0, :, :, 1] - product[1, :, :, 0]
    return jnp.stack([real_out, imag_out], 3)

def channelize(block, taps, table):
    span = taps.shape[0] - 1
    last_frames = block[:span]
    own_block = block[span:]
    own_part = transform(own_sum(own_block, taps).astype(jnp.bfloat16), table)
    carried_part = transform(carried_sum(last_frames, taps).astype(jnp.bfloat16), table)
    leading = own_part[:, :span] + carried_part
    return jnp.concatenate([leading, own_part[:, span:]], 1).astype(jnp.bfloat16)

def soft_weights(spectra, tolerance):
    count, frames, polars, parts, local = spectra.shape
    half = frames // 2
    values = spectra.astype(jnp.float32).reshape(count, 2, half, polars, parts, local)
    power = lax.optimization_barrier(jnp.sum(values * values, 4))
    first_sum = lax.optimization_barrier(jnp.sum(power, 2))
    second_sum = lax.optimization_barrier(jnp.sum(power * power, 2))
    size = float(half)
    kurtosis = (size + 1.0) / (size - 1.0) * (size * second_sum / (first_sum * first_sum) - 1.0)
    deviation = (kurtosis - 1.0) / tolerance[:, None, None, None]
    soft = 1.0 / (1.0 + deviation * deviation)
    weighted = values * soft[:, :, None, :, None, :]
    return weighted.astype(jnp.bfloat16).reshape(count, frames, polars, parts, local)

def reference(voltages, taps, sk_tolerance, station_coords, pointings, station_flags):
    frames_all = voltages.shape[0]
    span = TAPS - 1
    table = fourier_table(CHAN, NFFT)
    scale = 1.0 / math.sqrt(STATIONS)

    def one_block(index):
        own = lax.dynamic_slice_in_dim(voltages, index * F_DEV, F_DEV, 0)
        back = jnp.maximum(index * F_DEV - span, 0).astype(jnp.int32)
        prior = lax.dynamic_slice_in_dim(voltages, back, span, 0)
        prior = jnp.where(index > 0, prior, jnp.zeros_like(prior))
        return channelize(jnp.concatenate([prior, own], 0), taps, table)
    spectra = lax.map(one_block, jnp.arange(frames_all // F_DEV, dtype=jnp.int32))
    spectra = jnp.moveaxis(spectra, 0, 1).reshape(CHAN, frames_all, 2, 2, STATIONS)

    def one_channel(inputs):
        channel, values, tolerance = inputs
        weighted = soft_weights(values[None], tolerance[None])[0]
        weights = steering(channel[None], station_coords, station_flags, pointings, scale)[0]
        grouped = weighted.astype(jnp.float32).reshape(frames_all, 2, 2, N_STN, S_DEV)
        weight_groups = weights.astype(jnp.float32).reshape(2, N_STN, S_DEV, 2 * BEAMS)
        partial_value = jnp.einsum('tprgs,rgsj->gtpj', grouped, weight_groups)
        partial_value = lax.optimization_barrier(partial_value.astype(jnp.bfloat16)).astype(jnp.float32)
        beam = lax.optimization_barrier(jnp.sum(partial_value, 0))
        squares = (beam * beam).reshape(frames_all // INTEG, INTEG, 2, 2, BEAMS)
        return lax.optimization_barrier(jnp.sum(squares, (1, 2, 3))) / (2.0 * INTEG)
    return lax.map(one_channel, (jnp.arange(CHAN, dtype=jnp.int32), spectra, sk_tolerance))
```

```python
import functools
import math

import jax
import jax.numpy as jnp
from jax import lax
from jax.experimental import pallas as pl
from jax.experimental.pallas import tpu as pltpu
from jax.sharding import PartitionSpec as P

INTEG = 16
FINE = 16
LANES = 128
LIMIT = 60 * 1024 * 1024


def divides_evenly(v_count, h_count):
    return v_count == h_count and v_count > 4 and v_count % 2 == 0


def tap_sums(rows, count):
    if not divides_evenly(count, len(rows)):
        return list(rows)
    half = count // 2
    low, high = rows[:half], rows[half:]
    both = [a + b for a, b in zip(low, high)]
    return tap_sums(low, half) + tap_sums(high, half) + tap_sums(both, half)


def convolve(values, gains, at=0):
    count = len(values)
    if count <= 4 or count % 2:
        out = [None] * (2 * count - 1)
        rows = [gains(at + k) for k in range(count)]
        for f in range(count):
            for k in range(count):
                term = values[f] * rows[k]
                out[f + k] = term if out[f + k] is None else out[f + k] + term
        return out, at + count
    half = count // 2
    low, high = values[:half], values[half:]
    sums = [a + b for a, b in zip(low, high)]
    rows = at
    step = sum_rows(half)
    last, _ = convolve(high, gains, rows + step)
    first, _ = convolve(low, gains, rows)
    bias = []
    for i in range(2 * half - 1):
        both = first[i] + last[i]
        spot = half + i
        if spot < 2 * half - 1:
            both = first[spot] - both
        elif spot >= 2 * half:
            both = last[spot - 2 * half] - both
        else:
            both = -both
        bias.append(both)
    middle, _ = convolve(sums, gains, rows + 2 * step)
    middle = [m + b for m, b in zip(middle, bias)]
    return first[:half] + middle + last[half - 1 :], rows + 3 * step


def sum_rows(count):
    return count if count <= 4 or count % 2 else 3 * sum_rows(count // 2)


def turning_points(channels, points):
    columns = jnp.arange(points, dtype=jnp.int32)

    def pair(rows):
        residue = rows[:, None] * columns[None, :] % points
        angle = 2.0 * math.pi / points * residue.astype(jnp.float32)
        return jnp.cos(angle), jnp.sin(angle)

    factor = 1.0 / math.sqrt(points)
    coarse = [x * factor for x in pair(jnp.arange(channels // FINE, dtype=jnp.int32) * FINE)]
    return *coarse, *pair(jnp.arange(FINE, dtype=jnp.int32))


def lane_order(x, local):
    share = LANES // local
    sets = x.shape[0] // (share * local)
    split = x.reshape(sets, share // 2, 2, local // 8, 8, *x.shape[1:])
    return jnp.swapaxes(split, 2, 3).reshape(x.shape)


def steering(first, coords, flags, pointings, scale, local):
    coords, flags = lane_order(coords, local), lane_order(flags, local)
    offsets = coords[:, 0:1] * pointings[None, :, 0] + coords[:, 1:2] * pointings[None, :, 1]
    gain = ((1 - flags).astype(jnp.float32) * scale)[:, None]

    def turn(residue):
        angle = 2.0 * math.pi / 65536.0 * (residue % 65536).astype(jnp.float32)
        return jnp.cos(angle), jnp.sin(angle)

    pr, pi = turn((first + 1) * offsets)
    rr, ri = turn(offsets)
    return pr * gain, pi * gain, rr, ri


def beam_powers(tile, tolerance, weight, left_ref, blocks, groups, local):
    rows = left_ref.shape[1] // blocks
    tiles = rows // 2
    turned = lax.broadcasted_iota(jnp.int32, (rows, 1), 0) < tiles
    beams = weight.shape[1] // 2
    share = LANES // local
    frames = tiles * share
    windows = 2
    half = blocks // windows
    size = float(half * frames)

    lane = lax.broadcasted_iota(jnp.int32, (1, LANES), 1)
    kind = lane // (2 * local) * 2 + lane // 8 % 2

    def moved(x, source, target):
        pairs = target // 2 - source // 2
        shift = (pairs * 2 * local + (target % 2 - source % 2) * 8) % LANES
        return pltpu.roll(x, shift, 1) if shift else x

    def chosen(pieces):
        out = pieces[0]
        for q in range(1, share):
            out = jnp.where(kind == q, pieces[q], out)
        return out

    def folded(x):
        totals = []
        for q in range(share):
            total = x
            for k in range(share):
                if k != q:
                    total = total + moved(x, k, q)
            totals.append(total)
        return chosen(totals)

    first, second = [], []
    for w in range(windows):
        for g in range(groups):
            s1 = jnp.zeros((rows, LANES), jnp.float32)
            s2 = jnp.zeros((rows, LANES), jnp.float32)
            for b in range(w * half, (w + 1) * half):
                v = tile(b, g)
                power = v * v
                power = power + pltpu.roll(power, tiles, 0)
                s1 = s1 + power
                s2 = s2 + power * power
            first.append(jnp.sum(s1, 0, keepdims=True) * 0.5)
            second.append(jnp.sum(s2, 0, keepdims=True) * 0.5)
    first = folded(jnp.concatenate(first, 0))
    second = folded(jnp.concatenate(second, 0))
    kurtosis = (size + 1.0) / (size - 1.0) * (size * second / (first * first) - 1.0)
    deviation = (kurtosis - 1.0) / tolerance
    soft = 1.0 / (1.0 + deviation * deviation)
    for b in range(blocks):
        w = b // half
        pieces = [tile(b, g) * soft[w * groups + g : w * groups + g + 1] for g in range(groups)]
        for k in range(share):
            for at in range(0, groups, share):
                mixed = chosen([moved(pieces[at + q], k, q) for q in range(share)])
                column = at * local
                left_ref[k, b * rows : (b + 1) * rows, column : column + LANES] = mixed.astype(jnp.bfloat16)
    result = [None] * blocks
    for k in range(share):
        beam = jnp.dot(left_ref[k], weight, preferred_element_type=jnp.float32)
        for b in range(blocks):
            block = beam[b * rows : (b + 1) * rows]
            crossed = pltpu.roll(block[:, beams:], tiles, 0)
            value = block[:, :beams] + jnp.where(turned, -crossed, crossed)
            squares = value * value
            result[b] = squares if result[b] is None else result[b] + squares
    return jnp.concatenate([jnp.sum(r, 0, keepdims=True) for r in result], 0)


def whole_kernel(
    blocks, groups, owned, local, polars,
    tol_ref, pr_ref, pi_ref, rr_ref, ri_ref, taps_ref, cc_ref, cs_ref, fc_ref, fs_ref, volt_ref, out_ref,
    volt, sums, table, x_ref, own, acc, carried, came, spread, outgoing, arrived, weights, left, real, imag,
    power, beams_out, beams_in,
    volt_sem, carry_send, carry_recv, send_sem, recv_sem, beam_send, beam_recv,
):
    units, _, count, rows, _ = arrived.shape
    _, frames, parts, sub, chunk = volt.shape
    chunks, outs, _ = table.shape
    tiles = own.shape[1]
    channels = outs // 2
    halves = units // polars
    slots = groups * count
    devices = blocks * groups
    beams = pr_ref.shape[1]
    row_blocks = sub // 8
    lane_blocks = chunk // LANES
    share = max(8, row_blocks)
    pieces = parts * lane_blocks * row_blocks // share
    tm, stn = lax.axis_index("tm"), lax.axis_index("stn")
    me = tm * groups + stn

    def loop(start, stop, body):
        lax.fori_loop(start, stop, lambda k, unused: (body(k), unused)[1], 0)

    def load(n):
        u, i = n // chunks, lax.rem(n, chunks)
        station = pl.multiple_of(lax.rem(u, halves) * sub, sub)
        sample = pl.multiple_of(i * chunk, chunk)
        return pltpu.make_async_copy(
            volt_ref.at[:, :, u // halves, pl.ds(station, sub), pl.ds(sample, chunk)],
            volt.at[lax.rem(n, 2)],
            volt_sem.at[lax.rem(n, 2)],
        )

    def carry(u):
        return pltpu.make_async_remote_copy(
            src_ref=carried.at[u],
            dst_ref=came.at[u],
            send_sem=carry_send.at[u],
            recv_sem=carry_recv.at[u],
            device_id={"tm": lax.rem(tm + 1, blocks), "stn": stn},
            device_id_type=pl.DeviceIdType.MESH,
        )

    def parcel(u, k, arriving):
        to = lax.rem(me + k, devices)
        spot = lax.rem(me + devices - k, devices) if arriving else me
        return pltpu.make_async_remote_copy(
            src_ref=outgoing.at[u, pl.ds(to * count, count)],
            dst_ref=arrived.at[u, spot],
            send_sem=send_sem.at[u, k],
            recv_sem=recv_sem.at[u, spot],
            device_id={"tm": to // groups, "stn": lax.rem(to, groups)},
            device_id_type=pl.DeviceIdType.MESH,
        )

    def tabulated(i):
        at = pl.ds(pl.multiple_of(i * chunk, chunk), chunk)

        def step(n):
            a, b = cc_ref[pl.ds(n, 1), at], cs_ref[pl.ds(n, 1), at]
            c, d = fc_ref[:, at], fs_ref[:, at]
            cosine = a * c - b * d
            sine = b * c + a * d
            over = pl.ds(pl.multiple_of(n * FINE, FINE), FINE)
            under = pl.ds(pl.multiple_of(channels + n * FINE, FINE), FINE)
            table[i, over, :chunk] = cosine.astype(jnp.bfloat16)
            table[i, over, chunk:] = sine.astype(jnp.bfloat16)
            table[i, under, :chunk] = (-sine).astype(jnp.bfloat16)
            table[i, under, chunk:] = cosine.astype(jnp.bfloat16)

        loop(0, channels // FINE, step)

    def filtered(slot, i, j):
        for t in range(share):
            eight = t % row_blocks
            rest = j * (share // row_blocks) + t // row_blocks
            part = rest // lane_blocks
            shift = rest % lane_blocks * LANES
            lane = pl.multiple_of(shift, LANES)
            sample = pl.multiple_of(i * chunk + shift, LANES)
            column = pl.multiple_of(part * chunk + shift, LANES)
            row, low = eight // 2 * 16, eight % 2 * 8
            values = [
                volt[slot, f, part, row : row + 16, pl.ds(lane, LANES)].astype(jnp.float32)[low : low + 8]
                for f in range(frames)
            ]
            out, _ = convolve(values, lambda k: sums[k : k + 1, pl.ds(sample, LANES)])
            out.append(jnp.zeros((8, LANES), jnp.float32))
            for f in range(0, 2 * frames, 2):
                at = (f // 2 * row_blocks + eight) * 16
                pair = jnp.concatenate([out[f], out[f + 1]], 0).astype(jnp.bfloat16)
                x_ref[at : at + 16, pl.ds(column, LANES)] = pair

    def multiplied(u, i):
        product = lax.dot_general(
            table[i], x_ref[...], (((1,), (1,)), ((), ())), preferred_element_type=jnp.float32
        )
        for t in range(tiles):
            own[u % 2, t] = own[u % 2, t] + product[:, t * LANES : (t + 1) * LANES]
            acc[t] = acc[t] + product[:, (tiles + t) * LANES : (tiles + t + 1) * LANES]

    block = math.lcm(owned, 16)
    pitch = block + 8

    def combined(u):
        def step(i):
            for part in range(2):
                for t in range(tiles):
                    at = pl.ds(pl.multiple_of(part * channels + i * block, 16), block)
                    total = own[u % 2, t, at, :] + came[u, t, at, :].astype(jnp.float32)
                    base = (part * tiles + t) * pitch
                    spread[base : base + block, :] = total
            for c in range(block):
                values = spread[pl.ds(c, rows, pitch), :].astype(jnp.bfloat16)
                slot = c // owned * slots + c % owned
                outgoing[u, i * (block // owned) * slots + slot] = values

        loop(0, channels // block, step)

    def finished(u):
        @pl.when(tm > 0)
        def _():
            carry(u).wait_recv()

        combined(u)
        loop(1, devices, lambda k: parcel(u, k, False).start())
        arrived[u, me] = outgoing[u, pl.ds(me * count, count)]

    load(0).start()
    prepared = tap_sums([taps_ref[k : k + 1, :] for k in range(frames)], frames)
    for k, row in enumerate(prepared):
        sums[k : k + 1, :] = row

    @pl.when(tm == 0)
    def _():
        came[...] = jnp.zeros_like(came)

    if slots > owned:
        outgoing[...] = jnp.zeros_like(outgoing)

    def unit(u):
        own[u % 2] = jnp.zeros(own.shape[1:], jnp.float32)
        acc[...] = jnp.zeros_like(acc)

        def step(i):
            n = u * chunks + i
            load(n).wait()

            @pl.when(n + 1 < units * chunks)
            def _():
                load(n + 1).start()

            @pl.when(u == 0)
            def _():
                tabulated(i)

            loop(0, pieces, lambda j: filtered(lax.rem(n, 2), i, j))
            multiplied(u, i)

        loop(0, chunks, step)
        for t in range(tiles):
            carried[u, t] = acc[t].astype(jnp.bfloat16)

        @pl.when(u > 0)
        def _():
            finished(u - 1)

        @pl.when(tm < blocks - 1)
        def _():
            carry(u).start()

    loop(0, units, unit)

    real[...] = pr_ref[...]
    imag[...] = pi_ref[...]

    def turn(c):
        a, b, e, d = real[...], imag[...], rr_ref[...], ri_ref[...]
        weights[c, :, :beams] = a.astype(jnp.bfloat16)
        weights[c, :, beams:] = b.astype(jnp.bfloat16)
        real[...] = a * e - b * d
        imag[...] = a * d + b * e

    loop(0, count, turn)
    finished(units - 1)
    together = 2 if count % 2 == 0 else 1
    depth = left.shape[0] // 2

    def beamed(p):
        for h in range(halves):
            loop(1, devices, lambda k: parcel(p * halves + h, k, True).wait_recv())

        def step(n):
            for o in range(together):
                c = n * together + o

                def tile(b, g):
                    source = arrived[p * halves + g % halves, b * groups + g // halves, c]
                    return source.astype(jnp.float32)

                tolerance = jnp.full((1, LANES), tol_ref[c], jnp.float32)
                result = beam_powers(
                    tile, tolerance, weights[c], left.at[pl.ds(o * depth, depth)], blocks, groups * halves, sub
                )
                power[c] = result if p == 0 else power[c] + result

        loop(0, count // together, step)

    for p in range(polars):
        beamed(p)
    wide = beams // groups
    for c in range(count):
        total = power[c] * (1.0 / (2.0 * INTEG))
        for g in range(groups):
            beams_out[g, c] = total[:, g * wide : (g + 1) * wide]

    def portion(k, arriving):
        to = lax.rem(stn + k, groups)
        spot = lax.rem(stn + groups - k, groups) if arriving else stn
        return pltpu.make_async_remote_copy(
            src_ref=beams_out.at[to],
            dst_ref=beams_in.at[spot],
            send_sem=beam_send.at[k],
            recv_sem=beam_recv.at[spot],
            device_id={"tm": tm, "stn": to},
            device_id_type=pl.DeviceIdType.MESH,
        )

    for k in range(1, groups):
        portion(k, False).start()
    beams_in[stn] = beams_out[stn]

    @pl.when(tm < blocks - 1)
    def _():
        loop(0, units, lambda u: carry(u).wait_send())

    loop(0, units, lambda u: loop(1, devices, lambda k: parcel(u, k, False).wait_send()))
    for k in range(1, groups):
        portion(k, True).wait_recv()
    for i in range(owned):
        out_ref[i] = beams_in[i // count, i % count]
    for k in range(1, groups):
        portion(k, False).wait_send()


def whole_program(voltages, taps, turns, bases, tolerance, owned, blocks, groups, sub):
    frames, parts, polars, local, points = voltages.shape
    channels = owned * blocks
    chunk = min(512, points)
    chunks = points // chunk
    stations, beams = bases[0].shape
    count = tolerance.shape[0]
    tiles = frames * sub // LANES
    rows = 2 * tiles
    units = polars * (local // sub)
    devices = blocks * groups
    wide = beams // groups
    block = math.lcm(owned, 16)
    prepared = 3 ** max(0, int(math.log2(frames)) - 2) * min(frames, 4)
    vmem = pl.BlockSpec(memory_space=pltpu.VMEM)
    flops = 8 * units * frames * sub * channels * parts * points
    return pl.pallas_call(
        functools.partial(whole_kernel, blocks, groups, owned, local, polars),
        in_specs=[pl.BlockSpec(memory_space=pltpu.SMEM)] + [vmem] * 9 + [pl.BlockSpec(memory_space=pl.ANY)],
        out_specs=vmem,
        out_shape=jax.ShapeDtypeStruct((owned, blocks, wide), jnp.float32),
        scratch_shapes=[
            pltpu.VMEM((2, frames, parts, sub, chunk), jnp.bfloat16),
            pltpu.VMEM((prepared, points), jnp.float32),
            pltpu.VMEM((chunks, 2 * channels, parts * chunk), jnp.bfloat16),
            pltpu.VMEM((2 * frames * sub, parts * chunk), jnp.bfloat16),
            pltpu.VMEM((2, tiles, 2 * channels, LANES), jnp.float32),
            pltpu.VMEM((tiles, 2 * channels, LANES), jnp.float32),
            pltpu.VMEM((units, tiles, 2 * channels, LANES), jnp.bfloat16),
            pltpu.VMEM((units, tiles, 2 * channels, LANES), jnp.bfloat16),
            pltpu.VMEM((rows * (block + 8), LANES), jnp.float32),
            pltpu.VMEM((units, devices * count, rows, LANES), jnp.bfloat16),
            pltpu.VMEM((units, devices, count, rows, LANES), jnp.bfloat16),
            pltpu.VMEM((count, stations, 2 * beams), jnp.bfloat16),
            pltpu.VMEM((2 * (LANES // sub), blocks * rows, stations), jnp.bfloat16),
            pltpu.VMEM((stations, beams), jnp.float32),
            pltpu.VMEM((stations, beams), jnp.float32),
            pltpu.VMEM((count, blocks, beams), jnp.float32),
            pltpu.VMEM((groups, count, blocks, wide), jnp.float32),
            pltpu.VMEM((groups, count, blocks, wide), jnp.float32),
            pltpu.SemaphoreType.DMA((2,)),
            pltpu.SemaphoreType.DMA((units,)),
            pltpu.SemaphoreType.DMA((units,)),
            pltpu.SemaphoreType.DMA((units, devices)),
            pltpu.SemaphoreType.DMA((units, devices)),
            pltpu.SemaphoreType.DMA((groups,)),
            pltpu.SemaphoreType.DMA((groups,)),
        ],
        compiler_params=pltpu.CompilerParams(has_side_effects=True, vmem_limit_bytes=LIMIT),
        cost_estimate=pl.CostEstimate(flops=flops, bytes_accessed=40000000, transcendentals=0),
        name="station_beams",
    )(tolerance, *bases, taps, *turns, voltages)


def per_device(voltages, taps, sk_tolerance, station_coords, pointings, station_flags):
    frames, parts, polars, local, points = voltages.shape
    blocks = lax.axis_size("tm")
    groups = lax.axis_size("stn")
    owned = sk_tolerance.shape[0]
    channels = owned * blocks
    count = -(-owned // groups)
    spare = count * groups - owned
    sub = math.gcd(local, 32)
    share = LANES // sub
    assert frames == INTEG and taps.shape[0] == frames and channels % FINE == 0
    assert share % 2 == 0 and groups * local % LANES == 0
    scale = 1.0 / math.sqrt(groups * local)
    first = lax.axis_index("stn") * count
    start = lax.axis_index("tm") * owned + first
    turns = turning_points(channels, points)
    bases = steering(start, station_coords, station_flags, pointings, scale, sub)
    if spare:
        sk_tolerance = jnp.pad(sk_tolerance, (0, spare), constant_values=1.0)
    tolerance = lax.dynamic_slice_in_dim(sk_tolerance, first, count, 0)
    return whole_program(voltages, taps, turns, bases, tolerance, owned, blocks, groups, sub)


def solution(mesh):
    in_specs = (P("tm", None, None, "stn", None), P(), P("tm"), P(), P(), P())
    out_specs = P("tm", None, "stn")
    return jax.shard_map(
        per_device, mesh=mesh, in_specs=in_specs, out_specs=out_specs, check_vma=False
    )
```

```python
import functools
import math

import jax
import jax.numpy as jnp
from jax import lax
from jax.experimental import pallas as pl
from jax.experimental.pallas import tpu as pltpu
from jax.sharding import PartitionSpec as P

INTEG = 16
FINE = 16
LANES = 128
LIMIT = 60 * 1024 * 1024


def divides_evenly(v_count, h_count):
    return v_count == h_count and v_count > 4 and v_count % 2 == 0


def tap_sums(rows, count):
    if not divides_evenly(count, len(rows)):
        return list(rows)
    half = count // 2
    low, high = rows[:half], rows[half:]
    both = [a + b for a, b in zip(low, high)]
    return tap_sums(low, half) + tap_sums(high, half) + tap_sums(both, half)


def convolve(values, gains, at=0):
    count = len(values)
    if count <= 4 or count % 2:
        out = [None] * (2 * count - 1)
        rows = [gains(at + k) for k in range(count)]
        for f in range(count):
            for k in range(count):
                term = values[f] * rows[k]
                out[f + k] = term if out[f + k] is None else out[f + k] + term
        return out, at + count
    half = count // 2
    low, high = values[:half], values[half:]
    sums = [a + b for a, b in zip(low, high)]
    rows = at
    step = sum_rows(half)
    last, _ = convolve(high, gains, rows + step)
    first, _ = convolve(low, gains, rows)
    bias = []
    for i in range(2 * half - 1):
        both = first[i] + last[i]
        spot = half + i
        if spot < 2 * half - 1:
            both = first[spot] - both
        elif spot >= 2 * half:
            both = last[spot - 2 * half] - both
        else:
            both = -both
        bias.append(both)
    middle, _ = convolve(sums, gains, rows + 2 * step)
    middle = [m + b for m, b in zip(middle, bias)]
    return first[:half] + middle + last[half - 1 :], rows + 3 * step


def sum_rows(count):
    return count if count <= 4 or count % 2 else 3 * sum_rows(count // 2)


def turned(residue, bits):
    quarter = bits - 2
    turn = (residue + (1 << (quarter - 1))) >> quarter
    rest = (residue - (turn << quarter)).astype(jnp.float32) * (2.0 * math.pi / 2.0**bits)
    z = rest * rest
    sine, cosine = 0.0, 0.0
    for k in range(9, 0, -2):
        sine = (1.0 if k % 4 == 1 else -1.0) / math.factorial(k) + z * sine
    sine = rest * sine
    for k in range(10, -1, -2):
        cosine = (1.0 if k % 4 == 0 else -1.0) / math.factorial(k) + z * cosine
    odd = (turn & 1) == 1
    real = jnp.where(odd, sine, cosine)
    imag = jnp.where(odd, cosine, sine)
    real = jnp.where(((turn + 1) & 2) == 2, -real, real)
    imag = jnp.where((turn & 2) == 2, -imag, imag)
    return real, imag


def beam_powers(tile, tolerance, weight, left_ref, blocks, groups, local):
    rows = left_ref.shape[1] // blocks
    tiles = rows // 2
    turned = lax.broadcasted_iota(jnp.int32, (rows, 1), 0) < tiles
    beams = weight.shape[1] // 2
    share = LANES // local
    frames = tiles * share
    windows = 2
    half = blocks // windows
    size = float(half * frames)

    lane = lax.broadcasted_iota(jnp.int32, (1, LANES), 1)
    kind = lane // (2 * local) * 2 + lane // 8 % 2

    def moved(x, source, target):
        pairs = target // 2 - source // 2
        shift = (pairs * 2 * local + (target % 2 - source % 2) * 8) % LANES
        return pltpu.roll(x, shift, 1) if shift else x

    def chosen(pieces):
        out = pieces[0]
        for q in range(1, share):
            out = jnp.where(kind == q, pieces[q], out)
        return out

    def folded(x):
        totals = []
        for q in range(share):
            total = x
            for k in range(share):
                if k != q:
                    total = total + moved(x, k, q)
            totals.append(total)
        return chosen(totals)

    first, second = [], []
    for w in range(windows):
        for g in range(groups):
            s1 = jnp.zeros((rows, LANES), jnp.float32)
            s2 = jnp.zeros((rows, LANES), jnp.float32)
            for b in range(w * half, (w + 1) * half):
                v = tile(b, g)
                power = v * v
                power = power + pltpu.roll(power, tiles, 0)
                s1 = s1 + power
                s2 = s2 + power * power
            first.append(jnp.sum(s1, 0, keepdims=True) * 0.5)
            second.append(jnp.sum(s2, 0, keepdims=True) * 0.5)
    first = folded(jnp.concatenate(first, 0))
    second = folded(jnp.concatenate(second, 0))
    kurtosis = (size + 1.0) / (size - 1.0) * (size * second / (first * first) - 1.0)
    deviation = (kurtosis - 1.0) / tolerance
    soft = 1.0 / (1.0 + deviation * deviation)
    for b in range(blocks):
        w = b // half
        pieces = [tile(b, g) * soft[w * groups + g : w * groups + g + 1] for g in range(groups)]
        for k in range(share):
            for at in range(0, groups, share):
                mixed = chosen([moved(pieces[at + q], k, q) for q in range(share)])
                column = at * local
                left_ref[k, b * rows : (b + 1) * rows, column : column + LANES] = mixed.astype(jnp.bfloat16)
    result = [None] * blocks
    for k in range(share):
        beam = jnp.dot(left_ref[k], weight, preferred_element_type=jnp.float32)
        for b in range(blocks):
            block = beam[b * rows : (b + 1) * rows]
            crossed = pltpu.roll(block[:, beams:], tiles, 0)
            value = block[:, :beams] + jnp.where(turned, -crossed, crossed)
            squares = value * value
            result[b] = squares if result[b] is None else result[b] + squares
    return jnp.concatenate([jnp.sum(r, 0, keepdims=True) for r in result], 0)


def whole_kernel(
    blocks, groups, owned, local, polars,
    tol_ref, sites_ref, aims_ref, taps_ref, volt_ref, out_ref,
    volt, sums, coarse, fine, table, x_ref, own, carried, came, spread, outgoing, arrived, weights, left,
    real, imag, turn_real, turn_imag, power, beams_out, beams_in,
    volt_sem, carry_send, carry_recv, send_sem, recv_sem, beam_send, beam_recv,
):
    units, _, count, rows, _ = arrived.shape
    _, frames, parts, sub, chunk = volt.shape
    chunks, outs, _ = table.shape
    tiles = own.shape[0]
    channels = outs // 2
    halves = units // polars
    slots = groups * count
    devices = blocks * groups
    beams = aims_ref.shape[1]
    bits = (chunks * chunk).bit_length() - 1
    row_blocks = sub // 8
    lane_blocks = chunk // LANES
    share = max(8, row_blocks)
    pieces = parts * lane_blocks * row_blocks // share
    tm, stn = lax.axis_index("tm"), lax.axis_index("stn")
    me = tm * groups + stn

    def loop(start, stop, body):
        lax.fori_loop(start, stop, lambda k, unused: (body(k), unused)[1], 0)

    def load(n):
        u, i = n // chunks, lax.rem(n, chunks)
        station = pl.multiple_of(lax.rem(u, halves) * sub, sub)
        sample = pl.multiple_of(i * chunk, chunk)
        return pltpu.make_async_copy(
            volt_ref.at[:, :, u // halves, pl.ds(station, sub), pl.ds(sample, chunk)],
            volt.at[lax.rem(n, 2)],
            volt_sem.at[lax.rem(n, 2)],
        )

    def carry(u):
        return pltpu.make_async_remote_copy(
            src_ref=carried.at[u],
            dst_ref=came.at[u],
            send_sem=carry_send.at[u],
            recv_sem=carry_recv.at[u],
            device_id={"tm": lax.rem(tm + 1, blocks), "stn": stn},
            device_id_type=pl.DeviceIdType.MESH,
        )

    def parcel(u, k, arriving):
        to = lax.rem(me + k, devices)
        spot = lax.rem(me + devices - k, devices) if arriving else me
        return pltpu.make_async_remote_copy(
            src_ref=outgoing.at[u, pl.ds(to * count, count)],
            dst_ref=arrived.at[u, spot],
            send_sem=send_sem.at[u, k],
            recv_sem=recv_sem.at[u, spot],
            device_id={"tm": to // groups, "stn": lax.rem(to, groups)},
            device_id_type=pl.DeviceIdType.MESH,
        )

    def tabulated(i):
        def points_of(rows, stride):
            row = lax.broadcasted_iota(jnp.int32, (rows, chunk), 0) * stride
            column = lax.broadcasted_iota(jnp.int32, (rows, chunk), 1) + i * chunk
            return turned(row * column & ((1 << bits) - 1), bits)

        factor = 1.0 / math.sqrt(chunks * chunk)
        for k, values in enumerate(points_of(channels // FINE, FINE)):
            coarse[k] = values * factor
        for k, values in enumerate(points_of(FINE, 1)):
            fine[k] = values

        def step(n):
            a, b = coarse[0, pl.ds(n, 1), :], coarse[1, pl.ds(n, 1), :]
            c, d = fine[0], fine[1]
            cosine = a * c - b * d
            sine = b * c + a * d
            over = pl.ds(pl.multiple_of(n * FINE, FINE), FINE)
            under = pl.ds(pl.multiple_of(channels + n * FINE, FINE), FINE)
            table[i, over, :chunk] = cosine.astype(jnp.bfloat16)
            table[i, over, chunk:] = sine.astype(jnp.bfloat16)
            table[i, under, :chunk] = (-sine).astype(jnp.bfloat16)
            table[i, under, chunk:] = cosine.astype(jnp.bfloat16)

        loop(0, channels // FINE, step)

    def filtered(slot, i, j):
        for t in range(share):
            eight = t % row_blocks
            rest = j * (share // row_blocks) + t // row_blocks
            part = rest // lane_blocks
            shift = rest % lane_blocks * LANES
            lane = pl.multiple_of(shift, LANES)
            sample = pl.multiple_of(i * chunk + shift, LANES)
            column = pl.multiple_of(part * chunk + shift, LANES)
            row, low = eight // 2 * 16, eight % 2 * 8
            values = [
                volt[slot, f, part, row : row + 16, pl.ds(lane, LANES)].astype(jnp.float32)[low : low + 8]
                for f in range(frames)
            ]
            out, _ = convolve(values, lambda k: sums[k : k + 1, pl.ds(sample, LANES)])
            out.append(jnp.zeros((8, LANES), jnp.float32))
            for f in range(0, 2 * frames, 2):
                at = (f // 2 * row_blocks + eight) * 16
                pair = jnp.concatenate([out[f], out[f + 1]], 0).astype(jnp.bfloat16)
                x_ref[i, at : at + 16, pl.ds(column, LANES)] = pair

    def transformed(half):
        rows_of = pl.ds(half * frames * sub, frames * sub)
        product = None
        for i in range(chunks):
            piece = lax.dot_general(
                table[i], x_ref[i, rows_of, :], (((1,), (1,)), ((), ())), preferred_element_type=jnp.float32
            )
            product = piece if product is None else product + piece
        return [product[:, t * LANES : (t + 1) * LANES] for t in range(tiles)]

    block = math.lcm(owned, 16)
    pitch = block + 8

    def combined(u):
        def step(i):
            for part in range(2):
                for t in range(tiles):
                    at = pl.ds(pl.multiple_of(part * channels + i * block, 16), block)
                    total = own[t, at, :] + came[u, t, at, :].astype(jnp.float32)
                    base = (part * tiles + t) * pitch
                    spread[base : base + block, :] = total
            for c in range(block):
                values = spread[pl.ds(c, rows, pitch), :].astype(jnp.bfloat16)
                slot = c // owned * slots + c % owned
                outgoing[u, i * (block // owned) * slots + slot] = values

        loop(0, channels // block, step)

    def finished(u):
        @pl.when(tm > 0)
        def _():
            carry(u).wait_recv()

        combined(u)
        loop(1, devices, lambda k: parcel(u, k, False).start())
        arrived[u, me] = outgoing[u, pl.ds(me * count, count)]

    load(0).start()
    prepared = tap_sums([taps_ref[k : k + 1, :] for k in range(frames)], frames)
    for k, row in enumerate(prepared):
        sums[k : k + 1, :] = row

    @pl.when(tm == 0)
    def _():
        came[...] = jnp.zeros_like(came)

    if slots > owned:
        outgoing[...] = jnp.zeros_like(outgoing)

    def unit(u):
        def step(i):
            n = u * chunks + i
            load(n).wait()

            @pl.when(n + 1 < units * chunks)
            def _():
                load(n + 1).start()

            @pl.when(u == 0)
            def _():
                tabulated(i)

            loop(0, pieces, lambda j: filtered(lax.rem(n, 2), i, j))

        loop(0, chunks, step)

        @pl.when(u > 0)
        def _():
            finished(u - 1)

        for t, part in enumerate(transformed(1)):
            carried[u, t] = part.astype(jnp.bfloat16)

        @pl.when(tm < blocks - 1)
        def _():
            carry(u).start()

        for t, part in enumerate(transformed(0)):
            own[t] = part

    loop(0, units, unit)

    scale = 1.0 / math.sqrt(groups * local)
    channel = tm * owned + stn * count + 1

    def steered(n):
        rest, eight = n // (2 * row_blocks), lax.rem(n, row_blocks)
        spot = (rest * row_blocks + eight) * 2 + lax.rem(n // row_blocks, 2)
        source = pl.ds(pl.multiple_of(n * 8, 8), 8)
        target = pl.ds(pl.multiple_of(spot * 8, 8), 8)
        site = sites_ref[source, :]
        offsets = site[:, 0:1] * aims_ref[0:1, :] + site[:, 1:2] * aims_ref[1:2, :]
        gain = (1 - site[:, 2:3]).astype(jnp.float32) * scale
        a, b = turned(channel * offsets & 65535, 16)
        real[target, :] = a * gain
        imag[target, :] = b * gain
        turn_real[target, :], turn_imag[target, :] = turned(offsets & 65535, 16)

    loop(0, groups * local // 8, steered)

    def turn(c):
        a, b, e, d = real[...], imag[...], turn_real[...], turn_imag[...]
        weights[c, :, :beams] = a.astype(jnp.bfloat16)
        weights[c, :, beams:] = b.astype(jnp.bfloat16)
        real[...] = a * e - b * d
        imag[...] = a * d + b * e

    loop(0, count, turn)
    finished(units - 1)
    together = 2 if count % 2 == 0 else 1
    depth = left.shape[0] // 2

    def beamed(p):
        for h in range(halves):
            loop(1, devices, lambda k: parcel(p * halves + h, k, True).wait_recv())

        def step(n):
            for o in range(together):
                c = n * together + o

                def tile(b, g):
                    source = arrived[p * halves + g % halves, b * groups + g // halves, c]
                    return source.astype(jnp.float32)

                tolerance = jnp.full((1, LANES), tol_ref[stn * count + c], jnp.float32)
                result = beam_powers(
                    tile, tolerance, weights[c], left.at[pl.ds(o * depth, depth)], blocks, groups * halves, sub
                )
                power[c] = result if p == 0 else power[c] + result

        loop(0, count // together, step)

    for p in range(polars):
        beamed(p)
    wide = beams // groups
    for c in range(count):
        total = power[c] * (1.0 / (2.0 * INTEG))
        for g in range(groups):
            beams_out[g, c] = total[:, g * wide : (g + 1) * wide]

    def portion(k, arriving):
        to = lax.rem(stn + k, groups)
        spot = lax.rem(stn + groups - k, groups) if arriving else stn
        return pltpu.make_async_remote_copy(
            src_ref=beams_out.at[to],
            dst_ref=beams_in.at[spot],
            send_sem=beam_send.at[k],
            recv_sem=beam_recv.at[spot],
            device_id={"tm": tm, "stn": to},
            device_id_type=pl.DeviceIdType.MESH,
        )

    for k in range(1, groups):
        portion(k, False).start()
    beams_in[stn] = beams_out[stn]

    @pl.when(tm < blocks - 1)
    def _():
        loop(0, units, lambda u: carry(u).wait_send())

    loop(0, units, lambda u: loop(1, devices, lambda k: parcel(u, k, False).wait_send()))
    for k in range(1, groups):
        portion(k, True).wait_recv()
    for i in range(owned):
        out_ref[i] = beams_in[i // count, i % count]
    for k in range(1, groups):
        portion(k, False).wait_send()


def whole_program(voltages, taps, sites, aims, tolerance, owned, blocks, groups, sub):
    frames, parts, polars, local, points = voltages.shape
    channels = owned * blocks
    chunk = min(512, points)
    chunks = points // chunk
    stations, beams = sites.shape[0], aims.shape[1]
    count = tolerance.shape[0] // groups
    tiles = frames * sub // LANES
    rows = 2 * tiles
    units = polars * (local // sub)
    devices = blocks * groups
    wide = beams // groups
    block = math.lcm(owned, 16)
    prepared = 3 ** max(0, int(math.log2(frames)) - 2) * min(frames, 4)
    vmem = pl.BlockSpec(memory_space=pltpu.VMEM)
    flops = 8 * units * frames * sub * channels * parts * points
    return pl.pallas_call(
        functools.partial(whole_kernel, blocks, groups, owned, local, polars),
        in_specs=[pl.BlockSpec(memory_space=pltpu.SMEM)] + [vmem] * 3 + [pl.BlockSpec(memory_space=pl.ANY)],
        out_specs=vmem,
        out_shape=jax.ShapeDtypeStruct((owned, blocks, wide), jnp.float32),
        scratch_shapes=[
            pltpu.VMEM((2, frames, parts, sub, chunk), jnp.bfloat16),
            pltpu.VMEM((prepared, points), jnp.float32),
            pltpu.VMEM((2, channels // FINE, chunk), jnp.float32),
            pltpu.VMEM((2, FINE, chunk), jnp.float32),
            pltpu.VMEM((chunks, 2 * channels, parts * chunk), jnp.bfloat16),
            pltpu.VMEM((chunks, 2 * frames * sub, parts * chunk), jnp.bfloat16),
            pltpu.VMEM((tiles, 2 * channels, LANES), jnp.float32),
            pltpu.VMEM((units, tiles, 2 * channels, LANES), jnp.bfloat16),
            pltpu.VMEM((units, tiles, 2 * channels, LANES), jnp.bfloat16),
            pltpu.VMEM((rows * (block + 8), LANES), jnp.float32),
            pltpu.VMEM((units, devices * count, rows, LANES), jnp.bfloat16),
            pltpu.VMEM((units, devices, count, rows, LANES), jnp.bfloat16),
            pltpu.VMEM((count, stations, 2 * beams), jnp.bfloat16),
            pltpu.VMEM((2 * (LANES // sub), blocks * rows, stations), jnp.bfloat16),
            pltpu.VMEM((stations, beams), jnp.float32),
            pltpu.VMEM((stations, beams), jnp.float32),
            pltpu.VMEM((stations, beams), jnp.float32),
            pltpu.VMEM((stations, beams), jnp.float32),
            pltpu.VMEM((count, blocks, beams), jnp.float32),
            pltpu.VMEM((groups, count, blocks, wide), jnp.float32),
            pltpu.VMEM((groups, count, blocks, wide), jnp.float32),
            pltpu.SemaphoreType.DMA((2,)),
            pltpu.SemaphoreType.DMA((units,)),
            pltpu.SemaphoreType.DMA((units,)),
            pltpu.SemaphoreType.DMA((units, devices)),
            pltpu.SemaphoreType.DMA((units, devices)),
            pltpu.SemaphoreType.DMA((groups,)),
            pltpu.SemaphoreType.DMA((groups,)),
        ],
        compiler_params=pltpu.CompilerParams(has_side_effects=True, vmem_limit_bytes=LIMIT),
        cost_estimate=pl.CostEstimate(flops=flops, bytes_accessed=40000000, transcendentals=0),
        name="station_beams",
    )(tolerance, sites, aims, taps, voltages)


def per_device(voltages, taps, sk_tolerance, station_coords, pointings, station_flags):
    frames, parts, polars, local, points = voltages.shape
    blocks = lax.axis_size("tm")
    groups = lax.axis_size("stn")
    owned = sk_tolerance.shape[0]
    channels = owned * blocks
    count = -(-owned // groups)
    spare = count * groups - owned
    sub = math.gcd(local, 32)
    share = LANES // sub
    assert frames == INTEG and taps.shape[0] == frames and channels % FINE == 0
    assert share % 2 == 0 and groups * local % LANES == 0
    assert points & (points - 1) == 0
    sites = jnp.stack([station_coords[:, 0], station_coords[:, 1], station_flags], 1)
    if spare:
        sk_tolerance = jnp.pad(sk_tolerance, (0, spare), constant_values=1.0)
    return whole_program(voltages, taps, sites, pointings.T, sk_tolerance, owned, blocks, groups, sub)


def solution(mesh):
    in_specs = (P("tm", None, None, "stn", None), P(), P("tm"), P(), P(), P())
    out_specs = P("tm", None, "stn")
    return jax.shard_map(
        per_device, mesh=mesh, in_specs=in_specs, out_specs=out_specs, check_vma=False
    )
```

```python
import functools
import math

import jax
import jax.numpy as jnp
from jax import lax
from jax.experimental import pallas as pl
from jax.experimental.pallas import tpu as pltpu
from jax.sharding import PartitionSpec as P

INTEG = 16
FINE = 16
LANES = 128
LIMIT = 60 * 1024 * 1024


def divides_evenly(v_count, h_count):
    return v_count == h_count and v_count > 4 and v_count % 2 == 0


def tap_sums(rows, count):
    if not divides_evenly(count, len(rows)):
        return list(rows)
    half = count // 2
    low, high = rows[:half], rows[half:]
    both = [a + b for a, b in zip(low, high)]
    return tap_sums(low, half) + tap_sums(high, half) + tap_sums(both, half)


def convolve(values, gains, at=0):
    count = len(values)
    if count <= 4 or count % 2:
        out = [None] * (2 * count - 1)
        rows = [gains(at + k) for k in range(count)]
        for f in range(count):
            for k in range(count):
                term = values[f] * rows[k]
                out[f + k] = term if out[f + k] is None else out[f + k] + term
        return out, at + count
    half = count // 2
    low, high = values[:half], values[half:]
    sums = [a + b for a, b in zip(low, high)]
    rows = at
    step = sum_rows(half)
    last, _ = convolve(high, gains, rows + step)
    first, _ = convolve(low, gains, rows)
    bias = []
    for i in range(2 * half - 1):
        both = first[i] + last[i]
        spot = half + i
        if spot < 2 * half - 1:
            both = first[spot] - both
        elif spot >= 2 * half:
            both = last[spot - 2 * half] - both
        else:
            both = -both
        bias.append(both)
    middle, _ = convolve(sums, gains, rows + 2 * step)
    middle = [m + b for m, b in zip(middle, bias)]
    return first[:half] + middle + last[half - 1 :], rows + 3 * step


def sum_rows(count):
    return count if count <= 4 or count % 2 else 3 * sum_rows(count // 2)


def turned(residue, bits):
    quarter = bits - 2
    turn = (residue + (1 << (quarter - 1))) >> quarter
    rest = (residue - (turn << quarter)).astype(jnp.float32) * (2.0 * math.pi / 2.0**bits)
    z = rest * rest
    sine, cosine = 0.0, 0.0
    for k in range(9, 0, -2):
        sine = (1.0 if k % 4 == 1 else -1.0) / math.factorial(k) + z * sine
    sine = rest * sine
    for k in range(10, -1, -2):
        cosine = (1.0 if k % 4 == 0 else -1.0) / math.factorial(k) + z * cosine
    odd = (turn & 1) == 1
    real = jnp.where(odd, sine, cosine)
    imag = jnp.where(odd, cosine, sine)
    real = jnp.where(((turn + 1) & 2) == 2, -real, real)
    imag = jnp.where((turn & 2) == 2, -imag, imag)
    return real, imag


def beam_powers(tile, tolerance, weight, left_ref, blocks, groups, local):
    rows = left_ref.shape[1] // blocks
    tiles = rows // 2
    turned = lax.broadcasted_iota(jnp.int32, (rows, 1), 0) < tiles
    beams = weight.shape[1] // 2
    share = LANES // local
    frames = tiles * share
    windows = 2
    half = blocks // windows
    size = float(half * frames)

    lane = lax.broadcasted_iota(jnp.int32, (1, LANES), 1)
    kind = lane // (2 * local) * 2 + lane // 8 % 2

    def moved(x, source, target):
        pairs = target // 2 - source // 2
        shift = (pairs * 2 * local + (target % 2 - source % 2) * 8) % LANES
        return pltpu.roll(x, shift, 1) if shift else x

    def chosen(pieces):
        out = pieces[0]
        for q in range(1, share):
            out = jnp.where(kind == q, pieces[q], out)
        return out

    def folded(x):
        totals = []
        for q in range(share):
            total = x
            for k in range(share):
                if k != q:
                    total = total + moved(x, k, q)
            totals.append(total)
        return chosen(totals)

    first, second = [], []
    for w in range(windows):
        for g in range(groups):
            s1 = jnp.zeros((rows, LANES), jnp.float32)
            s2 = jnp.zeros((rows, LANES), jnp.float32)
            for b in range(w * half, (w + 1) * half):
                v = tile(b, g)
                power = v * v
                power = power + pltpu.roll(power, tiles, 0)
                s1 = s1 + power
                s2 = s2 + power * power
            first.append(jnp.sum(s1, 0, keepdims=True) * 0.5)
            second.append(jnp.sum(s2, 0, keepdims=True) * 0.5)
    first = folded(jnp.concatenate(first, 0))
    second = folded(jnp.concatenate(second, 0))
    kurtosis = (size + 1.0) / (size - 1.0) * (size * second / (first * first) - 1.0)
    deviation = (kurtosis - 1.0) / tolerance
    soft = 1.0 / (1.0 + deviation * deviation)
    for b in range(blocks):
        w = b // half
        pieces = [tile(b, g) * soft[w * groups + g : w * groups + g + 1] for g in range(groups)]
        for k in range(share):
            for at in range(0, groups, share):
                mixed = chosen([moved(pieces[at + q], k, q) for q in range(share)])
                column = at * local
                left_ref[k, b * rows : (b + 1) * rows, column : column + LANES] = mixed.astype(jnp.bfloat16)
    result = [None] * blocks
    for k in range(share):
        beam = jnp.dot(left_ref[k], weight, preferred_element_type=jnp.float32)
        for b in range(blocks):
            block = beam[b * rows : (b + 1) * rows]
            crossed = pltpu.roll(block[:, beams:], tiles, 0)
            value = block[:, :beams] + jnp.where(turned, -crossed, crossed)
            squares = value * value
            result[b] = squares if result[b] is None else result[b] + squares
    return jnp.concatenate([jnp.sum(r, 0, keepdims=True) for r in result], 0)


def whole_kernel(
    blocks, groups, owned, local, polars,
    tol_ref, sites_ref, aims_ref, taps_ref, volt_ref, out_ref,
    volt, sums, coarse, fine, table, x_ref, own, carried, came, spread, outgoing, arrived, weights, left,
    real, imag, turn_real, turn_imag, power, beams_out, beams_in,
    volt_sem, carry_send, carry_recv, send_sem, recv_sem, beam_send, beam_recv,
):
    units, _, count, rows, _ = arrived.shape
    _, frames, parts, sub, chunk = volt.shape
    chunks, outs, _ = table.shape
    tiles = own.shape[0]
    channels = outs // 2
    halves = units // polars
    slots = groups * count
    devices = blocks * groups
    beams = aims_ref.shape[1]
    bits = (chunks * chunk).bit_length() - 1
    row_blocks = sub // 8
    lane_blocks = chunk // LANES
    share = max(8, row_blocks)
    pieces = parts * lane_blocks * row_blocks // share
    tm, stn = lax.axis_index("tm"), lax.axis_index("stn")
    me = tm * groups + stn

    def loop(start, stop, body):
        lax.fori_loop(start, stop, lambda k, unused: (body(k), unused)[1], 0)

    def load(n):
        u, i = n // chunks, lax.rem(n, chunks)
        station = pl.multiple_of(lax.rem(u, halves) * sub, sub)
        sample = pl.multiple_of(i * chunk, chunk)
        return pltpu.make_async_copy(
            volt_ref.at[:, :, u // halves, pl.ds(station, sub), pl.ds(sample, chunk)],
            volt.at[lax.rem(n, 2)],
            volt_sem.at[lax.rem(n, 2)],
        )

    def carry(u):
        return pltpu.make_async_remote_copy(
            src_ref=carried.at[u],
            dst_ref=came.at[u],
            send_sem=carry_send.at[u],
            recv_sem=carry_recv.at[u],
            device_id={"tm": lax.rem(tm + 1, blocks), "stn": stn},
            device_id_type=pl.DeviceIdType.MESH,
        )

    def parcel(u, k, arriving):
        to = lax.rem(me + k, devices)
        spot = lax.rem(me + devices - k, devices) if arriving else me
        return pltpu.make_async_remote_copy(
            src_ref=outgoing.at[u, pl.ds(to * count, count)],
            dst_ref=arrived.at[u, spot],
            send_sem=send_sem.at[u, k],
            recv_sem=recv_sem.at[u, spot],
            device_id={"tm": to // groups, "stn": lax.rem(to, groups)},
            device_id_type=pl.DeviceIdType.MESH,
        )

    def tabulated(i):
        def points_of(rows, stride):
            row = lax.broadcasted_iota(jnp.int32, (rows, chunk), 0) * stride
            column = lax.broadcasted_iota(jnp.int32, (rows, chunk), 1) + i * chunk
            return turned(row * column & ((1 << bits) - 1), bits)

        factor = 1.0 / math.sqrt(chunks * chunk)
        for k, values in enumerate(points_of(channels // FINE, FINE)):
            coarse[k] = values * factor
        for k, values in enumerate(points_of(FINE, 1)):
            fine[k] = values

        def step(n):
            a, b = coarse[0, pl.ds(n, 1), :], coarse[1, pl.ds(n, 1), :]
            c, d = fine[0], fine[1]
            cosine = a * c - b * d
            sine = b * c + a * d
            over = pl.ds(pl.multiple_of(n * FINE, FINE), FINE)
            under = pl.ds(pl.multiple_of(channels + n * FINE, FINE), FINE)
            table[i, over, :chunk] = cosine.astype(jnp.bfloat16)
            table[i, over, chunk:] = sine.astype(jnp.bfloat16)
            table[i, under, :chunk] = (-sine).astype(jnp.bfloat16)
            table[i, under, chunk:] = cosine.astype(jnp.bfloat16)

        loop(0, channels // FINE, step)

    def filtered(slot, i, j):
        for t in range(share):
            eight = t % row_blocks
            rest = j * (share // row_blocks) + t // row_blocks
            part = rest // lane_blocks
            shift = rest % lane_blocks * LANES
            lane = pl.multiple_of(shift, LANES)
            sample = pl.multiple_of(i * chunk + shift, LANES)
            column = pl.multiple_of(part * chunk + shift, LANES)
            row, low = eight // 2 * 16, eight % 2 * 8
            values = [
                volt[slot, f, part, row : row + 16, pl.ds(lane, LANES)].astype(jnp.float32)[low : low + 8]
                for f in range(frames)
            ]
            out, _ = convolve(values, lambda k: sums[k : k + 1, pl.ds(sample, LANES)])
            out.append(jnp.zeros((8, LANES), jnp.float32))
            for f in range(0, 2 * frames, 2):
                at = (f // 2 * row_blocks + eight) * 16
                pair = jnp.concatenate([out[f], out[f + 1]], 0).astype(jnp.bfloat16)
                x_ref[i, at : at + 16, pl.ds(column, LANES)] = pair

    def transformed(half):
        rows_of = pl.ds(half * frames * sub, frames * sub)
        product = None
        for i in range(chunks):
            piece = lax.dot_general(
                table[i], x_ref[i, rows_of, :], (((1,), (1,)), ((), ())), preferred_element_type=jnp.float32
            )
            product = piece if product is None else product + piece
        return [product[:, t * LANES : (t + 1) * LANES] for t in range(tiles)]

    block = math.lcm(owned, 16)
    pitch = block + 8

    def combined(u):
        def step(i):
            for part in range(2):
                for t in range(tiles):
                    at = pl.ds(pl.multiple_of(part * channels + i * block, 16), block)
                    total = own[t, at, :] + came[u, t, at, :].astype(jnp.float32)
                    base = (part * tiles + t) * pitch
                    spread[base : base + block, :] = total
            for c in range(block):
                values = spread[pl.ds(c, rows, pitch), :].astype(jnp.bfloat16)
                slot = c // owned * slots + c % owned
                outgoing[u, i * (block // owned) * slots + slot] = values

        loop(0, channels // block, step)

    def finished(u):
        @pl.when(tm > 0)
        def _():
            carry(u).wait_recv()

        combined(u)
        loop(1, devices, lambda k: parcel(u, k, False).start())
        arrived[u, me] = outgoing[u, pl.ds(me * count, count)]

    load(0).start()
    prepared = tap_sums([taps_ref[k : k + 1, :] for k in range(frames)], frames)
    for k, row in enumerate(prepared):
        sums[k : k + 1, :] = row

    @pl.when(tm == 0)
    def _():
        came[...] = jnp.zeros_like(came)

    if slots > owned:
        outgoing[...] = jnp.zeros_like(outgoing)

    def unit(u):
        def step(i):
            n = u * chunks + i
            load(n).wait()

            @pl.when(n + 1 < units * chunks)
            def _():
                load(n + 1).start()

            @pl.when(u == 0)
            def _():
                tabulated(i)

            loop(0, pieces, lambda j: filtered(lax.rem(n, 2), i, j))

        loop(0, chunks, step)

        @pl.when(u == 1)
        def _():
            finished(u - 1)

        for t, part in enumerate(transformed(1)):
            carried[u, t] = part.astype(jnp.bfloat16)

        @pl.when(tm < blocks - 1)
        def _():
            carry(u).start()

        @pl.when(u > 1)
        def _():
            finished(u - 1)

        for t, part in enumerate(transformed(0)):
            own[t] = part

    loop(0, units, unit)

    scale = 1.0 / math.sqrt(groups * local)
    channel = tm * owned + stn * count + 1

    def steered(n):
        rest, eight = n // (2 * row_blocks), lax.rem(n, row_blocks)
        spot = (rest * row_blocks + eight) * 2 + lax.rem(n // row_blocks, 2)
        source = pl.ds(pl.multiple_of(n * 8, 8), 8)
        target = pl.ds(pl.multiple_of(spot * 8, 8), 8)
        site = sites_ref[source, :]
        offsets = site[:, 0:1] * aims_ref[0:1, :] + site[:, 1:2] * aims_ref[1:2, :]
        gain = (1 - site[:, 2:3]).astype(jnp.float32) * scale
        a, b = turned(channel * offsets & 65535, 16)
        real[target, :] = a * gain
        imag[target, :] = b * gain
        turn_real[target, :], turn_imag[target, :] = turned(offsets & 65535, 16)

    loop(0, groups * local // 8, steered)

    def turn(c):
        a, b, e, d = real[...], imag[...], turn_real[...], turn_imag[...]
        weights[c, :, :beams] = a.astype(jnp.bfloat16)
        weights[c, :, beams:] = b.astype(jnp.bfloat16)
        real[...] = a * e - b * d
        imag[...] = a * d + b * e

    loop(0, count, turn)
    finished(units - 1)
    together = math.gcd(count, 4)
    depth = left.shape[0] // 4

    def beamed(p):
        for h in range(halves):
            loop(1, devices, lambda k: parcel(p * halves + h, k, True).wait_recv())

        def step(n):
            for o in range(together):
                c = n * together + o

                def tile(b, g):
                    source = arrived[p * halves + g % halves, b * groups + g // halves, c]
                    return source.astype(jnp.float32)

                tolerance = jnp.full((1, LANES), tol_ref[stn * count + c], jnp.float32)
                result = beam_powers(
                    tile, tolerance, weights[c], left.at[pl.ds(o * depth, depth)], blocks, groups * halves, sub
                )
                power[c] = result if p == 0 else power[c] + result

        loop(0, count // together, step)

    for p in range(polars):
        beamed(p)
    wide = beams // groups
    for c in range(count):
        total = power[c] * (1.0 / (2.0 * INTEG))
        for g in range(groups):
            beams_out[g, c] = total[:, g * wide : (g + 1) * wide]

    def portion(k, arriving):
        to = lax.rem(stn + k, groups)
        spot = lax.rem(stn + groups - k, groups) if arriving else stn
        return pltpu.make_async_remote_copy(
            src_ref=beams_out.at[to],
            dst_ref=beams_in.at[spot],
            send_sem=beam_send.at[k],
            recv_sem=beam_recv.at[spot],
            device_id={"tm": tm, "stn": to},
            device_id_type=pl.DeviceIdType.MESH,
        )

    for k in range(1, groups):
        portion(k, False).start()
    beams_in[stn] = beams_out[stn]

    @pl.when(tm < blocks - 1)
    def _():
        loop(0, units, lambda u: carry(u).wait_send())

    loop(0, units, lambda u: loop(1, devices, lambda k: parcel(u, k, False).wait_send()))
    for k in range(1, groups):
        portion(k, True).wait_recv()
    for i in range(owned):
        out_ref[i] = beams_in[i // count, i % count]
    for k in range(1, groups):
        portion(k, False).wait_send()


def whole_program(voltages, taps, sites, aims, tolerance, owned, blocks, groups, sub):
    frames, parts, polars, local, points = voltages.shape
    channels = owned * blocks
    chunk = min(512, points)
    chunks = points // chunk
    stations, beams = sites.shape[0], aims.shape[1]
    count = tolerance.shape[0] // groups
    tiles = frames * sub // LANES
    rows = 2 * tiles
    units = polars * (local // sub)
    devices = blocks * groups
    wide = beams // groups
    block = math.lcm(owned, 16)
    prepared = 3 ** max(0, int(math.log2(frames)) - 2) * min(frames, 4)
    vmem = pl.BlockSpec(memory_space=pltpu.VMEM)
    flops = 8 * units * frames * sub * channels * parts * points
    return pl.pallas_call(
        functools.partial(whole_kernel, blocks, groups, owned, local, polars),
        in_specs=[pl.BlockSpec(memory_space=pltpu.SMEM)] + [vmem] * 3 + [pl.BlockSpec(memory_space=pl.ANY)],
        out_specs=vmem,
        out_shape=jax.ShapeDtypeStruct((owned, blocks, wide), jnp.float32),
        scratch_shapes=[
            pltpu.VMEM((2, frames, parts, sub, chunk), jnp.bfloat16),
            pltpu.VMEM((prepared, points), jnp.float32),
            pltpu.VMEM((2, channels // FINE, chunk), jnp.float32),
            pltpu.VMEM((2, FINE, chunk), jnp.float32),
            pltpu.VMEM((chunks, 2 * channels, parts * chunk), jnp.bfloat16),
            pltpu.VMEM((chunks, 2 * frames * sub, parts * chunk), jnp.bfloat16),
            pltpu.VMEM((tiles, 2 * channels, LANES), jnp.float32),
            pltpu.VMEM((units, tiles, 2 * channels, LANES), jnp.bfloat16),
            pltpu.VMEM((units, tiles, 2 * channels, LANES), jnp.bfloat16),
            pltpu.VMEM((rows * (block + 8), LANES), jnp.float32),
            pltpu.VMEM((units, devices * count, rows, LANES), jnp.bfloat16),
            pltpu.VMEM((units, devices, count, rows, LANES), jnp.bfloat16),
            pltpu.VMEM((count, stations, 2 * beams), jnp.bfloat16),
            pltpu.VMEM((4 * (LANES // sub), blocks * rows, stations), jnp.bfloat16),
            pltpu.VMEM((stations, beams), jnp.float32),
            pltpu.VMEM((stations, beams), jnp.float32),
            pltpu.VMEM((stations, beams), jnp.float32),
            pltpu.VMEM((stations, beams), jnp.float32),
            pltpu.VMEM((count, blocks, beams), jnp.float32),
            pltpu.VMEM((groups, count, blocks, wide), jnp.float32),
            pltpu.VMEM((groups, count, blocks, wide), jnp.float32),
            pltpu.SemaphoreType.DMA((2,)),
            pltpu.SemaphoreType.DMA((units,)),
            pltpu.SemaphoreType.DMA((units,)),
            pltpu.SemaphoreType.DMA((units, devices)),
            pltpu.SemaphoreType.DMA((units, devices)),
            pltpu.SemaphoreType.DMA((groups,)),
            pltpu.SemaphoreType.DMA((groups,)),
        ],
        compiler_params=pltpu.CompilerParams(has_side_effects=True, vmem_limit_bytes=LIMIT),
        cost_estimate=pl.CostEstimate(flops=flops, bytes_accessed=40000000, transcendentals=0),
        name="station_beams",
    )(tolerance, sites, aims, taps, voltages)


def per_device(voltages, taps, sk_tolerance, station_coords, pointings, station_flags):
    frames, parts, polars, local, points = voltages.shape
    blocks = lax.axis_size("tm")
    groups = lax.axis_size("stn")
    owned = sk_tolerance.shape[0]
    channels = owned * blocks
    count = -(-owned // groups)
    spare = count * groups - owned
    sub = math.gcd(local, 32)
    share = LANES // sub
    assert frames == INTEG and taps.shape[0] == frames and channels % FINE == 0
    assert share % 2 == 0 and groups * local % LANES == 0
    assert points & (points - 1) == 0
    sites = jnp.stack([station_coords[:, 0], station_coords[:, 1], station_flags], 1)
    if spare:
        sk_tolerance = jnp.pad(sk_tolerance, (0, spare), constant_values=1.0)
    return whole_program(voltages, taps, sites, pointings.T, sk_tolerance, owned, blocks, groups, sub)


def solution(mesh):
    in_specs = (P("tm", None, None, "stn", None), P(), P("tm"), P(), P(), P())
    out_specs = P("tm", None, "stn")
    return jax.shard_map(
        per_device, mesh=mesh, in_specs=in_specs, out_specs=out_specs, check_vma=False
    )
```
